256 devices in a mesh: member: 4 (over y, x), node: 64 (over z, core).
Axes of the slice: x: 2, y: 2, z: 32, core: 2. Of those that a mesh axis runs over, the one named last changes fastest.
The devices are a block of a 4x8x32 slice.
Arguments:
- conditioning: bfloat16 [168, 262144], P(None, ('member', 'node')), parts along dimension 1, may hold values from -6 to 6
- target_state: float32 [84, 262144], P(None, ('member', 'node')), parts along dimension 1, may hold values from -6 to 6
- noise_sample: float32 [84, 262144], P(None, ('member', 'node')), parts along dimension 1, may hold values from -6 to 6
- step_index: int32 [4], P('member'), parts along dimension 0, may hold values from 0 to 19
- mesh_features: float32 [3, 40960], P(None, 'node'), may hold values from -1 to 1
- edge_geometry: float32 [4, 262144], P(None, 'node'), may hold values from -6 to 6
- edge_slot: int32 [262144], P('node'), may hold values from 0 to 1023, as said below
- edge_receiver: int32 [262144], P('node'), may hold values from 0 to 639
- send_rows: int32 [4096, 16], P('node'), may hold values from 0 to 1023
- edge_count: int32 [64], P('node'), may hold values from 1503 to 4096, as said below
- embed_weight: bfloat16 [252, 512], replicated, may hold values from -0.375 to 0.375
- mesh_weight: float32 [3, 512], replicated, may hold values from -3.5 to 3.5
- geom_weight: float32 [4, 512], replicated, may hold values from -3 to 3
- sender_weight: bfloat16 [512, 512], P('node'), may hold values from -0.15625 to 0.15625
- edge_weight: bfloat16 [512, 512], P('node'), may hold values from -0.15625 to 0.15625
- receiver_weight: bfloat16 [512, 512], P('node'), may hold values from -0.15625 to 0.15625
- message_weight: bfloat16 [512, 512], P('node'), may hold values from -0.25 to 0.25
- node_weight: bfloat16 [1024, 512], P('node'), may hold values from -0.1875 to 0.1875
- output_weight: bfloat16 [512, 512], P('node'), may hold values from -0.25 to 0.25
- noise_weight: float32 [32, 512], replicated, may hold values from -1 to 1
- film_weight: bfloat16 [512, 2048], replicated, may hold values from -0.25 to 0.25
Outputs:
- mesh_latent: bfloat16 [40960, 2048], P('node', 'member'), parts along dimension 1
The draws below stay inside these ranges and needn't reach their ends.
There are 4 independent parts, one for each index of `member`. The reference program is written for one: setup_inputs(seed, part) draws one part's arguments, and reference() takes and returns one part's arrays. A program takes and returns all parts, laid end to end along the dimension named above; an argument that names none is the same for every part. Nothing has to cross between parts.
Inputs may be any that keep to these rules, and one draw needn't show every extreme that they name: `edge_slot`: on each device, the live slots name every entry of its 64 * 16 list at least once, or as many distinct entries as there are live slots where these are fewer. `edge_count`: the counts sum to 64 * 2048 and one device has all 4096 slots live.
All inputs are finite; a program needn't handle non-finite values.
Results may differ from the reference program's by a relative error of at most 0.0071.
Values may be sent and summed in bfloat16 or wider, within the bound.
No kernel may reach another device: no remote copies, remote signals or barrier semaphores. Data moves between devices by JAX's collectives and lax.ppermute only.
A program may use at most 64 MiB of HBM per device.

```python
import jax
import jax.numpy as jnp
from jax import lax

LAT = 512
VARS = 84
G_DEV = 1024
M_DEV = 640
E_DEV = 4096
CAP = 16
STEPS = 20
FREQ = 16
C_COND = 168
C_RAW = 252
GRID = 65536
MESH = 40960
EDGES = 262144
PAIRS = 4096
N_NODE = 64


def live_counts(key):
    base_key = jax.random.fold_in(key, 11)
    order_key, spread_key = jax.random.split(base_key)
    order = jax.random.permutation(order_key, N_NODE).astype(jnp.int32)
    position = jnp.arange(N_NODE, dtype=jnp.int32)
    others = N_NODE - 1
    excess = E_DEV // 2
    share = excess // others
    remain = excess % others
    loss = share + (position - 1 < remain).astype(jnp.int32)
    spread = jax.random.randint(spread_key, (N_NODE,), 0, E_DEV // 8 + 1).astype(jnp.int32)
    following = jnp.where(position == N_NODE - 1, 1, position + 1).astype(jnp.int32)
    delta = spread - spread[following]
    placed = jnp.where(position == 0, E_DEV, E_DEV // 2 - loss + delta).astype(jnp.int32)
    return jnp.zeros((N_NODE,), jnp.int32).at[order].set(placed)


def draw_edge_count(key, part):
    return live_counts(key)


def draw_edge_slot(key, part):
    counts = live_counts(key)
    listed = N_NODE * CAP
    slot_key = jax.random.fold_in(key, 23)
    device_keys = jax.vmap(lambda index: jax.random.fold_in(slot_key, index))(jnp.arange(N_NODE, dtype=jnp.int32))

    def one_device(device_key, count):
        first_key, second_key = jax.random.split(device_key)
        order = jax.random.permutation(first_key, listed).astype(jnp.int32)
        extra = jax.random.randint(second_key, (E_DEV,), 0, listed).astype(jnp.int32)
        used = jnp.minimum(count, listed)
        position = jnp.arange(E_DEV, dtype=jnp.int32)
        pick = jnp.where(position < listed, position, extra % used)
        pick = jnp.minimum(pick, listed - 1)
        return order[pick]
    return jax.vmap(one_device)(device_keys, counts).reshape(N_NODE * E_DEV)


def plant(drawn, stream_key, smallest, high):
    longest = drawn.shape.index(max(drawn.shape))
    spots = []
    for shift in (0, 1):
        where = [jax.random.randint(jax.random.fold_in(stream_key, axis), (), 0, length) for axis, length in enumerate(drawn.shape)]
        where[longest] = (where[longest] + shift) % drawn.shape[longest]
        spots.append(tuple(where))
    return drawn.at[spots[0]].set(smallest).at[spots[1]].set(high)


def block_levels(key, shape, shards, least, largest):
    factor_of, own = 1.0, jax.random.fold_in(key, 6)
    for axis_at, blocks in shards:
        steps = jnp.exp(jax.random.uniform(jax.random.fold_in(own, axis_at), (blocks,), jnp.float32, least / len(shards), largest / len(shards)))
        factor_of = factor_of * jnp.repeat(steps, shape[axis_at] // blocks).reshape([-1 if axis == axis_at else 1 for axis in range(len(shape))])
    return factor_of


def gaussian(key, extent, width, limit, pieces=(), held_as=jnp.bfloat16):
    drawn = width * jax.random.normal(key, extent, jnp.float32)
    if pieces:
        drawn = drawn * block_levels(key, extent, pieces, -0.22, 0.18)
    return jnp.clip(drawn, -limit, limit).astype(held_as)


def setup_inputs(seed: int = 0, part: int = 0) -> dict:
    arg_keys = jax.random.split(jax.random.key(seed), 22)
    part_splits = jax.random.split(jax.random.fold_in(arg_keys[21], part), 22)
    return {
        "conditioning": gaussian(part_splits[0], (C_COND, GRID), 1.0, 6.0, ((1, 64),)),
        "target_state": gaussian(part_splits[1], (VARS, GRID), 1.0, 6.0, ((1, 64),), jnp.float32),
        "noise_sample": gaussian(part_splits[2], (VARS, GRID), 1.0, 6.0, ((1, 64),), jnp.float32),
        "step_index": jax.random.randint(part_splits[3], (1,), 0, STEPS).astype(jnp.int32),
        "mesh_features": jnp.clip(jax.random.uniform(arg_keys[4], (3, MESH), jnp.float32, -1.0, 1.0) * block_levels(arg_keys[4], (3, MESH), ((1, 64),), -0.4, 0.0), -1.0, 1.0),
        "edge_geometry": gaussian(arg_keys[5], (4, EDGES), 1.0, 6.0, ((1, 64),), jnp.float32),
        "edge_slot": draw_edge_slot(jax.random.fold_in(arg_keys[21], 71), part),
        "edge_receiver": plant(jax.random.randint(arg_keys[7], (EDGES,), 0, M_DEV), jax.random.fold_in(arg_keys[7], 1), 0, M_DEV - 1).astype(jnp.int32),
        "send_rows": plant(jax.random.randint(arg_keys[8], (PAIRS, CAP), 0, G_DEV), jax.random.fold_in(arg_keys[8], 1), 0, G_DEV - 1).astype(jnp.int32),
        "edge_count": draw_edge_count(jax.random.fold_in(arg_keys[21], 71), part),
        "embed_weight": gaussian(arg_keys[10], (C_RAW, LAT), C_RAW ** -0.5, 0.375),
        "mesh_weight": gaussian(arg_keys[11], (3, LAT), 3 ** -0.5, 3.5, (), jnp.float32),
        "geom_weight": gaussian(arg_keys[12], (4, LAT), 4 ** -0.5, 3.0, (), jnp.float32),
        "sender_weight": gaussian(arg_keys[13], (LAT, LAT), (3 * LAT) ** -0.5, 0.15625, ((0, 64),)),
        "edge_weight": gaussian(arg_keys[14], (LAT, LAT), (3 * LAT) ** -0.5, 0.15625, ((0, 64),)),
        "receiver_weight": gaussian(arg_keys[15], (LAT, LAT), (3 * LAT) ** -0.5, 0.15625, ((0, 64),)),
        "message_weight": gaussian(arg_keys[16], (LAT, LAT), LAT ** -0.5, 0.25, ((0, 64),)),
        "node_weight": gaussian(arg_keys[17], (2 * LAT, LAT), (2 * LAT) ** -0.5, 0.1875, ((0, 64),)),
        "output_weight": gaussian(arg_keys[18], (LAT, LAT), LAT ** -0.5, 0.25, ((0, 64),)),
        "noise_weight": gaussian(arg_keys[19], (2 * FREQ, LAT), (2 * FREQ) ** -0.5, 1.0, (), jnp.float32),
        "film_weight": gaussian(arg_keys[20], (LAT, 4 * LAT), LAT ** -0.5, 0.25),
    }


sigma_top = 80.0
sigma_low = 0.03
rho_power = 7.0
norm_eps = 1e-05

def layer_norm(values):
    mean = lax.optimization_barrier(jnp.mean(values, axis=-1, keepdims=True))
    centred = values - mean
    var = lax.optimization_barrier(jnp.mean(centred * centred, axis=-1, keepdims=True))
    return centred * lax.rsqrt(var + norm_eps)

def noise_terms(step_index, noise_weight, film_weight):
    frac = step_index[0].astype(jnp.float32) / (STEPS - 1)
    upper = sigma_top ** (1.0 / rho_power)
    lower = sigma_low ** (1.0 / rho_power)
    sigma = (upper + frac * (lower - upper)) ** rho_power
    angle = 0.25 * jnp.log(sigma) * (jnp.arange(FREQ, dtype=jnp.float32) + 1.0)
    fourier = jnp.concatenate([jnp.sin(angle), jnp.cos(angle)])[None, :]
    cond = jax.nn.silu(jnp.dot(fourier, noise_weight, precision=lax.Precision.HIGHEST)).astype(jnp.bfloat16)
    film = jnp.dot(cond, film_weight, preferred_element_type=jnp.float32)
    return (sigma, film)

def reference(conditioning, target_state, noise_sample, step_index, mesh_features, edge_geometry, edge_slot, edge_receiver, send_rows, edge_count, embed_weight, mesh_weight, geom_weight, sender_weight, edge_weight, receiver_weight, message_weight, node_weight, output_weight, noise_weight, film_weight):
    sigma, film = noise_terms(step_index, noise_weight, film_weight)
    edge_scale = film[:, 0:LAT]
    edge_shift = film[:, LAT:2 * LAT]
    node_scale = film[:, 2 * LAT:3 * LAT]
    node_shift = film[:, 3 * LAT:4 * LAT]
    noisy = ((target_state + sigma * noise_sample) / jnp.sqrt(sigma * sigma + 1.0)).astype(jnp.bfloat16)
    raw = jnp.concatenate([conditioning, noisy], axis=0)
    grid_latent = jax.nn.silu(jnp.dot(raw.T, embed_weight, preferred_element_type=jnp.float32)).astype(jnp.bfloat16)
    mesh_embed = jax.nn.silu(jnp.dot(mesh_features.T, mesh_weight, precision=lax.Precision.HIGHEST)).astype(jnp.bfloat16)
    recv_proj = jnp.dot(mesh_embed, receiver_weight, preferred_element_type=jnp.float32).astype(jnp.bfloat16)
    edge_embed = jax.nn.silu(jnp.dot(edge_geometry.T, geom_weight, precision=lax.Precision.HIGHEST)).astype(jnp.bfloat16)
    tables = send_rows.reshape(N_NODE, N_NODE, CAP)
    bands = jnp.arange(N_NODE, dtype=jnp.int32)

    def one_device(device):
        table = lax.dynamic_index_in_dim(tables, device, 1, keepdims=False)
        grid_index = (bands[:, None] * G_DEV + table).reshape(N_NODE * CAP)
        start = (device * E_DEV).astype(jnp.int32)
        slots = lax.dynamic_slice_in_dim(edge_slot, start, E_DEV, 0)
        local_recv = lax.dynamic_slice_in_dim(edge_receiver, start, E_DEV, 0)
        embed_rows = lax.dynamic_slice_in_dim(edge_embed, start, E_DEV, 0)
        node_start = (device * M_DEV).astype(jnp.int32)
        proj_local = lax.dynamic_slice_in_dim(recv_proj, node_start, M_DEV, 0)
        mesh_local = lax.dynamic_slice_in_dim(mesh_embed, node_start, M_DEV, 0)
        sender_rows = grid_latent[grid_index[slots]]
        pre = jnp.dot(embed_rows, edge_weight, preferred_element_type=jnp.float32)
        pre = pre + jnp.dot(sender_rows, sender_weight, preferred_element_type=jnp.float32)
        pre = pre + proj_local[local_recv].astype(jnp.float32)
        hidden = jax.nn.silu(pre).astype(jnp.bfloat16)
        mixed = jnp.dot(hidden, message_weight, preferred_element_type=jnp.float32)
        message = layer_norm(mixed) * (1.0 + edge_scale) + edge_shift
        count = lax.dynamic_index_in_dim(edge_count, device, 0, keepdims=False)
        live = jnp.arange(E_DEV, dtype=jnp.int32) < count
        message = jnp.where(live[:, None], message, 0.0).astype(jnp.bfloat16)
        gathered = jax.ops.segment_sum(message.astype(jnp.float32), local_recv, num_segments=M_DEV).astype(jnp.bfloat16)
        joined = jnp.concatenate([mesh_local, gathered], axis=1)
        update = jax.nn.silu(jnp.dot(joined, node_weight, preferred_element_type=jnp.float32)).astype(jnp.bfloat16)
        result = jnp.dot(update, output_weight, preferred_element_type=jnp.float32)
        return (mesh_local.astype(jnp.float32) + layer_norm(result) * (1.0 + node_scale) + node_shift).astype(jnp.bfloat16)
    blocks = lax.map(one_device, bands)
    return blocks.reshape(MESH, LAT)
```

```python
import functools

import jax
import jax.numpy as jnp
from jax import lax
from jax.experimental import pallas as pl
from jax.experimental.pallas import tpu as pltpu
from jax.sharding import PartitionSpec as P

STEPS = 20

sigma_top = 80.0
sigma_low = 0.03
rho_power = 7.0
norm_eps = 1e-05

NEAR = 4
QUAD = 4
ROWS8 = ("sender", "edge", "recv", "message")

bf16 = jnp.bfloat16
f32 = jnp.float32


def silu(x):
    half = 0.5 * x
    return half + half * jnp.tanh(half)


def node_of(position, far):
    core, rest = divmod(position, NEAR * far)
    near, k = divmod(rest, far)
    return (near + NEAR * k) * 2 + core


def permute_rows(values, far, group):
    return jnp.concatenate(
        [
            values[node_of(p, far) * group : (node_of(p, far) + 1) * group]
            for p in range(2 * NEAR * far)
        ],
        axis=0,
    )


def norm_rows(values):
    mean = jnp.mean(values, axis=0, keepdims=True)
    centred = values - mean
    var = jnp.mean(centred * centred, axis=0, keepdims=True)
    return centred * lax.rsqrt(var + norm_eps)


def pick_kernel(noise_ref, cond_ref, target_ref, sample_ref, rows_ref, out_ref, raw_ref):
    sigma, scale = noise_ref[0], noise_ref[1]
    cond_rows, var_rows = cond_ref.shape[0], target_ref.shape[0]
    total = raw_ref.shape[0]
    raw_ref[total - 8 :, :] = jnp.zeros((8, raw_ref.shape[1]), f32)
    raw_ref[:cond_rows, :] = cond_ref[...].astype(f32)
    noisy = (target_ref[...] + sigma * sample_ref[...]) / scale
    raw_ref[cond_rows : cond_rows + var_rows, :] = noisy
    raw = raw_ref[...].astype(bf16)
    points = raw.shape[1]
    picks = out_ref.shape[0]
    step = min(256, picks)
    for start in range(0, picks, step):
        wanted = rows_ref[:, start : start + step]
        hot = jnp.where(
            lax.broadcasted_iota(jnp.int32, (points, step), 0) == wanted, 1.0, 0.0
        ).astype(bf16)
        got = jnp.dot(raw, hot, preferred_element_type=f32)
        out_ref[start : start + step, :] = got.T.astype(bf16)


def early_kernel(
    far,
    place_ref,
    raw_ref,
    geom_ref,
    geom_w_ref,
    mesh_ref,
    mesh_w_ref,
    recv_ref,
    pre_ref,
    sender_ref,
    message_ref,
    node_ref,
    output_ref,
    embed_ref,
    edge_ref,
    recv_w_ref,
    proj_ref,
):
    lanes = raw_ref.shape[-1]
    depth = NEAR * far * 8

    @pl.when(pl.program_id(0) == 0)
    def _():
        quarter, core = place_ref[0], place_ref[1]
        for c in range(2):
            for q in range(QUAD):
                t = core ^ c
                d = quarter ^ q
                u, v = (d >> 1, d & 1) if c == 0 else (d & 1, d >> 1)
                piece = raw_ref[t, u, v].astype(f32)
                cols = slice(c * depth, (c + 1) * depth)
                rows = slice(q * lanes, (q + 1) * lanes)

                def turned(first, count):
                    return piece[:, first : first + count, :].reshape(-1, lanes).T

                def spread(ref, values, where):
                    groups = lanes // 8
                    chips = groups // 2
                    ks = chips // NEAR
                    for c2 in range(2):
                        for near in range(NEAR):
                            block = jnp.concatenate(
                                [
                                    values[((near + NEAR * j) * 2 + c2) * 8 :][:8]
                                    for j in range(ks)
                                ],
                                axis=0,
                            )
                            at = (c2 * NEAR * far + near * far + q * ks) * 8
                            ref[at : at + 8 * ks, where] = block.astype(bf16)

                spread(sender_ref, turned(0, 8), cols)
                spread(edge_ref, turned(8, 8), cols)
                spread(recv_w_ref, turned(16, 8), cols)
                message_ref[rows, cols] = turned(24, 8).astype(bf16)
                spread(node_ref, turned(32, 16), slice(2 * c * depth, 2 * (c + 1) * depth))
                output_ref[rows, cols] = turned(48, 8).astype(bf16)
        embed = silu(jnp.dot(mesh_w_ref[...], mesh_ref[...], preferred_element_type=f32))
        embed_ref[...] = embed.astype(bf16)
        ordered = permute_rows(embed, far, 8).astype(bf16)
        proj_ref[...] = jnp.dot(
            recv_w_ref[...], ordered, preferred_element_type=f32
        ).astype(bf16)

    edges = geom_ref.shape[1]
    edge_embed = silu(
        jnp.dot(geom_w_ref[...], geom_ref[...], preferred_element_type=f32)
    ).astype(bf16)
    nodes = proj_ref.shape[1]
    hot = jnp.where(
        lax.broadcasted_iota(jnp.int32, (nodes, edges), 0) == recv_ref[...], 1.0, 0.0
    ).astype(bf16)
    pre = jnp.dot(edge_ref[...], edge_embed, preferred_element_type=f32)
    pre = pre + jnp.dot(proj_ref[...], hot, preferred_element_type=f32)
    pre_ref[...] = pre.astype(bf16)


def late_kernel(
    far,
    count_ref,
    arrived_ref,
    grid_w_ref,
    sender_ref,
    message_ref,
    node_ref,
    output_ref,
    embed_ref,
    film_ref,
    pre_ref,
    slot_ref,
    recv_ref,
    out_ref,
    table_ref,
    total_ref,
):
    step = pl.program_id(0)
    count = count_ref[0]

    @pl.when(step == 0)
    def _():
        latent = silu(
            lax.dot_general(
                grid_w_ref[...],
                arrived_ref[...],
                (((1,), (1,)), ((), ())),
                preferred_element_type=f32,
            )
        )
        ordered = permute_rows(latent, far, 8).astype(bf16)
        table_ref[...] = jnp.dot(
            sender_ref[...], ordered, preferred_element_type=f32
        ).astype(bf16)
        total_ref[...] = jnp.zeros_like(total_ref)

    edges = pre_ref.shape[1]
    start = step * edges

    @pl.when(start < count)
    def _():
        listed = table_ref.shape[1]
        nodes = total_ref.shape[1]
        hot = jnp.where(
            lax.broadcasted_iota(jnp.int32, (listed, edges), 0) == slot_ref[...], 1.0, 0.0
        ).astype(bf16)
        pre = pre_ref[...].astype(f32)
        pre = pre + jnp.dot(table_ref[...], hot, preferred_element_type=f32)
        hidden = silu(pre).astype(bf16)
        mixed = jnp.dot(message_ref[...], hidden, preferred_element_type=f32)
        message = norm_rows(mixed) * film_ref[:, 0:1] + film_ref[:, 1:2]
        message = message.astype(bf16)
        live = start + lax.broadcasted_iota(jnp.int32, (1, edges), 1) < count
        target = jnp.where(live, recv_ref[...], -1)
        home = jnp.where(
            lax.broadcasted_iota(jnp.int32, (nodes, edges), 0) == target, 1.0, 0.0
        ).astype(bf16)
        total_ref[...] += lax.dot_general(
            message, home, (((1,), (1,)), ((), ())), preferred_element_type=f32
        )

    @pl.when(step == pl.num_programs(0) - 1)
    def _():
        embed = embed_ref[...]
        joined = jnp.concatenate([embed, total_ref[...].astype(bf16)], axis=0)
        ordered = permute_rows(joined, far, 16)
        update = silu(jnp.dot(node_ref[...], ordered, preferred_element_type=f32)).astype(bf16)
        result = jnp.dot(output_ref[...], update, preferred_element_type=f32)
        latent = embed.astype(f32) + norm_rows(result) * film_ref[:, 2:3] + film_ref[:, 3:4]
        out_ref[...] = latent.T.astype(bf16)


def gather_weights(block, members, nodes):
    rows, width = block.shape
    lanes = width // QUAD
    chips = nodes // 2
    far = chips // NEAR
    quarter = lax.axis_index("member") % QUAD
    mine = lax.dynamic_slice_in_dim(block, quarter * lanes, lanes, 1)
    strided = [
        [(a + NEAR * k) * 2 + c for k in range(far)] for a in range(NEAR) for c in range(2)
    ]
    close = [
        [(a + NEAR * k) * 2 + c for a in range(NEAR)] for k in range(far) for c in range(2)
    ]
    held = lax.all_to_all(
        jnp.broadcast_to(mine[None], (far, rows, lanes)),
        "node",
        0,
        0,
        tiled=True,
        axis_index_groups=strided,
    )
    held = lax.all_to_all(
        jnp.broadcast_to(held[None], (NEAR, far, rows, lanes)),
        "node",
        0,
        0,
        tiled=True,
        axis_index_groups=close,
    )
    held = held.reshape(chips, rows, lanes)

    def swap(even, odd):
        return [
            (m * nodes + n, (m ^ (odd if n % 2 else even)) * nodes + n)
            for m in range(members)
            for n in range(nodes)
        ]

    for even, odd in ((1, 2), (2, 1)):
        other = lax.ppermute(held, ("member", "node"), swap(even, odd))
        held = jnp.stack([held, other])
    other = lax.ppermute(held, "node", [(n, n ^ 1) for n in range(nodes)])
    return jnp.stack([held, other])


def three_parts(values):
    high = lax.reduce_precision(values, 8, 7)
    rest = values - high
    middle = lax.reduce_precision(rest, 8, 7)
    low = rest - middle
    return high.astype(bf16), middle.astype(bf16), low.astype(bf16)


def exact_operands(weight, features):
    w1, w2, w3 = three_parts(weight.T)
    x1, x2, x3 = three_parts(features)
    left = jnp.concatenate([w1, w2, w1, w3, w2, w1], axis=1)
    right = jnp.concatenate([x1, x1, x2, x1, x2, x3], axis=0)
    pad = -left.shape[1] % 32
    return jnp.pad(left, ((0, 0), (0, pad))), jnp.pad(right, ((0, pad), (0, 0)))


def vmem(shape, index=None):
    if index is None:
        return pl.BlockSpec(shape, lambda i: (0,) * len(shape))
    return pl.BlockSpec(shape, index)


def per_device(
    members,
    nodes,
    conditioning,
    target_state,
    noise_sample,
    step_index,
    mesh_features,
    edge_geometry,
    edge_slot,
    edge_receiver,
    send_rows,
    edge_count,
    embed_weight,
    mesh_weight,
    geom_weight,
    sender_weight,
    edge_weight,
    receiver_weight,
    message_weight,
    node_weight,
    output_weight,
    noise_weight,
    film_weight,
):
    width = embed_weight.shape[1]
    chips = nodes // 2
    far = chips // NEAR
    block = jnp.concatenate(
        [sender_weight, edge_weight, receiver_weight, message_weight, node_weight, output_weight],
        axis=0,
    )
    weights = gather_weights(block, members, nodes)

    freqs = noise_weight.shape[0] // 2
    frac = step_index[0].astype(f32) / (STEPS - 1)
    upper = sigma_top ** (1.0 / rho_power)
    lower = sigma_low ** (1.0 / rho_power)
    sigma = (upper + frac * (lower - upper)) ** rho_power
    noise = jnp.stack([sigma, jnp.sqrt(sigma * sigma + 1.0)])

    picks = send_rows.size
    raw_rows = conditioning.shape[0] + target_state.shape[0]
    padded = raw_rows + -raw_rows % 16
    points = conditioning.shape[1]
    outgoing = pl.pallas_call(
        pick_kernel,
        out_shape=jax.ShapeDtypeStruct((picks, padded), bf16),
        in_specs=[pl.BlockSpec(memory_space=pltpu.SMEM)]
        + [pl.BlockSpec(memory_space=pltpu.VMEM)] * 4,
        out_specs=pl.BlockSpec(memory_space=pltpu.VMEM),
        scratch_shapes=[pltpu.VMEM((padded, points), f32)],
        cost_estimate=pl.CostEstimate(
            flops=2 * picks * points * padded, bytes_accessed=4 * picks * padded, transcendentals=0
        ),
        name="pick_rows",
    )(noise, conditioning, target_state, noise_sample, send_rows.reshape(1, picks))
    arrived = lax.all_to_all(
        outgoing.reshape(nodes, picks // nodes, padded), "node", 0, 0, tiled=True
    ).reshape(picks, padded)

    angle = 0.25 * jnp.log(sigma) * (jnp.arange(freqs, dtype=f32) + 1.0)
    fourier = jnp.concatenate([jnp.sin(angle), jnp.cos(angle)])[None, :]
    cond = jax.nn.silu(jnp.dot(fourier, noise_weight, precision=lax.Precision.HIGHEST)).astype(bf16)
    film = jnp.dot(cond, film_weight, preferred_element_type=f32).reshape(4, width)
    film = (film + jnp.array([1.0, 0.0, 1.0, 0.0], f32)[:, None]).T

    geom_w, geom = exact_operands(geom_weight, edge_geometry)
    geom_w = (
        geom_w.reshape(far, NEAR, 2, width // nodes, -1)
        .transpose(2, 1, 0, 3, 4)
        .reshape(geom_w.shape)
    )
    mesh_w, mesh = exact_operands(mesh_weight, mesh_features)
    grid_w = jnp.pad(embed_weight.T, ((0, 0), (0, padded - raw_rows)))

    edges = edge_slot.shape[0]
    mesh_count = mesh_features.shape[1]
    step = min(512, edges)
    steps = edges // step
    place = jnp.stack(
        [lax.axis_index("member") % QUAD, lax.axis_index("node") % 2]
    ).astype(jnp.int32)
    slots = edge_slot.reshape(1, edges)
    receivers = edge_receiver.reshape(1, edges)
    smem = pl.BlockSpec(memory_space=pltpu.SMEM)
    lane_block = lambda i: (0, i)

    square = jax.ShapeDtypeStruct((width, width), bf16)
    pre, sender_t, message_t, node_t, output_t, mesh_embed = pl.pallas_call(
        functools.partial(early_kernel, far),
        grid=(steps,),
        out_shape=(
            jax.ShapeDtypeStruct((width, edges), bf16),
            square,
            square,
            jax.ShapeDtypeStruct((width, 2 * width), bf16),
            square,
            jax.ShapeDtypeStruct((width, mesh_count), bf16),
        ),
        in_specs=[
            smem,
            vmem(weights.shape),
            vmem((geom.shape[0], step), lane_block),
            vmem(geom_w.shape),
            vmem(mesh.shape),
            vmem(mesh_w.shape),
            vmem((1, step), lane_block),
        ],
        out_specs=(
            vmem((width, step), lane_block),
            vmem((width, width)),
            vmem((width, width)),
            vmem((width, 2 * width)),
            vmem((width, width)),
            vmem((width, mesh_count)),
        ),
        scratch_shapes=[
            pltpu.VMEM((width, width), bf16),
            pltpu.VMEM((width, width), bf16),
            pltpu.VMEM((width, mesh_count), bf16),
        ],
        cost_estimate=pl.CostEstimate(
            flops=2 * edges * width * (width + mesh_count + 256),
            bytes_accessed=2 * edges * width + 8 * weights.size,
            transcendentals=edges * width,
        ),
        name="early",
    )(place, weights, geom, geom_w, mesh, mesh_w, receivers)

    return pl.pallas_call(
        functools.partial(late_kernel, far),
        grid=(steps,),
        out_shape=jax.ShapeDtypeStruct((mesh_count, width), bf16),
        in_specs=[
            smem,
            vmem(arrived.shape),
            vmem(grid_w.shape),
            vmem((width, width)),
            vmem((width, width)),
            vmem((width, 2 * width)),
            vmem((width, width)),
            vmem((width, mesh_count)),
            vmem(film.shape),
            vmem((width, step), lane_block),
            vmem((1, step), lane_block),
            vmem((1, step), lane_block),
        ],
        out_specs=vmem((mesh_count, width)),
        scratch_shapes=[
            pltpu.VMEM((width, picks), bf16),
            pltpu.VMEM((width, mesh_count), f32),
        ],
        cost_estimate=pl.CostEstimate(
            flops=2 * edges * width * (width + mesh_count + picks),
            bytes_accessed=2 * edges * width,
            transcendentals=edges * width,
        ),
        name="late",
    )(
        edge_count,
        arrived,
        grid_w,
        sender_t,
        message_t,
        node_t,
        output_t,
        mesh_embed,
        film,
        pre,
        slots,
        receivers,
    )


def solution(mesh):
    placed = (
        P(None, ("member", "node")),
        P(None, ("member", "node")),
        P(None, ("member", "node")),
        P("member"),
        P(None, "node"),
        P(None, "node"),
        P("node"),
        P("node"),
        P("node", None),
        P("node"),
        P(),
        P(),
        P(),
        P("node", None),
        P("node", None),
        P("node", None),
        P("node", None),
        P("node", None),
        P("node", None),
        P(),
        P(),
    )
    return jax.shard_map(
        functools.partial(per_device, mesh.shape["member"], mesh.shape["node"]),
        mesh=mesh,
        in_specs=placed,
        out_specs=P("node", "member"),
        check_vma=False,
    )
```

```python
import functools

import jax
import jax.numpy as jnp
from jax import lax
from jax.experimental import pallas as pl
from jax.experimental.pallas import tpu as pltpu
from jax.sharding import PartitionSpec as P


STEPS = 20

sigma_top = 80.0
sigma_low = 0.03
rho_power = 7.0
norm_eps = 1e-05

NEAR = 4
QUAD = 4

bf16 = jnp.bfloat16
f32 = jnp.float32


def silu(x):
    half = 0.5 * x
    return half + half * jnp.tanh(half)


def node_of(position, far):
    core, rest = divmod(position, NEAR * far)
    near, k = divmod(rest, far)
    return (near + NEAR * k) * 2 + core


def permute_rows(values, far, group):
    return jnp.concatenate(
        [
            values[node_of(p, far) * group : (node_of(p, far) + 1) * group]
            for p in range(2 * NEAR * far)
        ],
        axis=0,
    )


def norm_rows(values):
    mean = jnp.mean(values, axis=0, keepdims=True)
    centred = values - mean
    var = jnp.mean(centred * centred, axis=0, keepdims=True)
    return centred * lax.rsqrt(var + norm_eps)


def pick_kernel(noise_ref, cond_ref, target_ref, sample_ref, rows_ref, out_ref, raw_ref):
    sigma, scale = noise_ref[0], noise_ref[1]
    cond_rows, var_rows = cond_ref.shape[0], target_ref.shape[0]
    total = raw_ref.shape[0]
    raw_ref[total - 8 :, :] = jnp.zeros((8, raw_ref.shape[1]), f32)
    raw_ref[:cond_rows, :] = cond_ref[...].astype(f32)
    noisy = (target_ref[...] + sigma * sample_ref[...]) / scale
    raw_ref[cond_rows : cond_rows + var_rows, :] = noisy
    raw = raw_ref[...].astype(bf16)
    points = raw.shape[1]
    picks = out_ref.shape[0]
    step = min(256, picks)
    for start in range(0, picks, step):
        wanted = rows_ref[:, start : start + step]
        hot = jnp.where(
            lax.broadcasted_iota(jnp.int32, (points, step), 0) == wanted, 1.0, 0.0
        ).astype(bf16)
        got = jnp.dot(raw, hot, preferred_element_type=f32)
        out_ref[start : start + step, :] = got.T.astype(bf16)


def pack_kernel(*refs):
    blocks, out_ref = refs[:-1], refs[-1]
    lanes = out_ref.shape[2]
    quarter = lax.axis_index("member") & (QUAD - 1)
    at = pl.multiple_of(quarter * lanes, lanes)
    rows = jnp.concatenate([b[:, pl.ds(at, lanes)].astype(f32) for b in blocks], axis=0)
    rows = rows.astype(bf16)
    for k in range(out_ref.shape[0]):
        out_ref[k] = rows


def early_kernel(
    far,
    first_w_ref,
    geom_ref,
    mesh_ref,
    recv_ref,
    *refs,
):
    pieces = refs[:8]
    pre_ref, sender_ref, message_ref, node_ref, output_ref, embed_ref = refs[8:14]
    edge_ref, recv_w_ref, proj_ref = refs[14:]
    lanes = pieces[0].shape[-1]
    depth = NEAR * far * 8
    groups = lanes // 8
    ks = groups // 2 // NEAR
    corners = geom_ref.shape[0]

    def first_layer(ref, begin):
        total = 0.0
        for k in range(ref.shape[0]):
            total = total + first_w_ref[:, begin + k : begin + k + 1] * ref[k : k + 1, :]
        return silu(total)

    @pl.when(pl.program_id(0) == 0)
    def _():
        quarter = lax.axis_index("member") & (QUAD - 1)
        node = lax.axis_index("node")
        core = node & 1
        chip = (node >> 1) & (NEAR - 1)
        for number, piece_ref in enumerate(pieces):
            c = core ^ (number // 4)
            mask = (0, 1 + c, 2 - c, 3)[number % 4]
            q = quarter ^ mask
            piece = jnp.concatenate(
                [piece_ref[chip ^ near].astype(f32) for near in range(NEAR)], axis=0
            )
            cols = pl.ds(pl.multiple_of(c * depth, depth), depth)
            wide = pl.ds(pl.multiple_of(c * 2 * depth, 2 * depth), 2 * depth)
            rows = pl.ds(pl.multiple_of(q * lanes, lanes), lanes)

            def turned(first, count):
                return piece[:, first : first + count, :].reshape(-1, lanes).T

            def spread(ref, values, where):
                for c2 in range(2):
                    for near in range(NEAR):
                        block = jnp.concatenate(
                            [
                                values[((near + NEAR * j) * 2 + c2) * 8 :][:8]
                                for j in range(ks)
                            ],
                            axis=0,
                        )
                        at = (c2 * NEAR * far + near * far) * 8 + q * (8 * ks)
                        at = pl.multiple_of(at, 8 * ks)
                        ref[pl.ds(at, 8 * ks), where] = block.astype(bf16)

            spread(sender_ref, turned(0, 8), cols)
            spread(edge_ref, turned(8, 8), cols)
            spread(recv_w_ref, turned(16, 8), cols)
            message_ref[rows, cols] = turned(24, 8).astype(bf16)
            spread(node_ref, turned(32, 16), wide)
            output_ref[rows, cols] = turned(48, 8).astype(bf16)
        embed = first_layer(mesh_ref, corners)
        embed_ref[...] = embed.astype(bf16)
        ordered = permute_rows(embed, far, 8).astype(bf16)
        proj_ref[...] = jnp.dot(
            recv_w_ref[...], ordered, preferred_element_type=f32
        ).astype(bf16)

    edges = geom_ref.shape[1]
    edge_embed = permute_rows(first_layer(geom_ref, 0), far, 8).astype(bf16)
    nodes = proj_ref.shape[1]
    hot = jnp.where(
        lax.broadcasted_iota(jnp.int32, (nodes, edges), 0) == recv_ref[...], 1.0, 0.0
    ).astype(bf16)
    pre = jnp.dot(edge_ref[...], edge_embed, preferred_element_type=f32)
    pre = pre + jnp.dot(proj_ref[...], hot, preferred_element_type=f32)
    pre_ref[0] = pre.astype(bf16)


def late_kernel(
    far,
    count_ref,
    film_ref,
    slot_ref,
    recv_ref,
    arrived_hbm,
    grid_w_hbm,
    sender_hbm,
    pre_hbm,
    message_hbm,
    embed_hbm,
    node_hbm,
    output_hbm,
    out_ref,
    arrived_ref,
    grid_w_ref,
    sender_ref,
    pre_ref,
    message_ref,
    embed_ref,
    node_ref,
    output_ref,
    table_ref,
    total_ref,
    sems,
    pre_sems,
):
    count = count_ref[0]
    steps, _, edges = pre_ref.shape
    whole = [
        pltpu.make_async_copy(src, dst, sems.at[k])
        for k, (src, dst) in enumerate(
            (
                (arrived_hbm, arrived_ref),
                (grid_w_hbm, grid_w_ref),
                (sender_hbm, sender_ref),
                (message_hbm, message_ref),
                (embed_hbm, embed_ref),
                (node_hbm, node_ref),
                (output_hbm, output_ref),
            )
        )
    ]

    def part(k):
        return pltpu.make_async_copy(pre_hbm.at[k], pre_ref.at[k], pre_sems.at[k])

    for copy in whole[:4]:
        copy.start()
    for k in range(steps):
        part(k).start()
    for copy in whole[4:]:
        copy.start()

    total_ref[...] = jnp.zeros_like(total_ref)
    whole[0].wait()
    whole[1].wait()
    latent = silu(
        lax.dot_general(
            grid_w_ref[...],
            arrived_ref[...],
            (((1,), (1,)), ((), ())),
            preferred_element_type=f32,
        )
    )
    ordered = permute_rows(latent, far, 8).astype(bf16)
    whole[2].wait()
    table_ref[...] = jnp.dot(sender_ref[...], ordered, preferred_element_type=f32).astype(bf16)
    whole[3].wait()

    listed = table_ref.shape[1]
    nodes = total_ref.shape[1]

    def add_block(k, carry):
        start = k * edges
        lanes = pl.ds(pl.multiple_of(start, edges), edges)
        hot = jnp.where(
            lax.broadcasted_iota(jnp.int32, (listed, edges), 0) == slot_ref[:, lanes], 1.0, 0.0
        ).astype(bf16)
        pre = pre_ref[k].astype(f32)
        pre = pre + jnp.dot(table_ref[...], hot, preferred_element_type=f32)
        hidden = silu(pre).astype(bf16)
        mixed = jnp.dot(message_ref[...], hidden, preferred_element_type=f32)
        message = norm_rows(mixed) * film_ref[:, 0:1] + film_ref[:, 1:2]
        message = message.astype(bf16)
        live = start + lax.broadcasted_iota(jnp.int32, (1, edges), 1) < count
        target = jnp.where(live, recv_ref[:, lanes], -1)
        home = jnp.where(
            lax.broadcasted_iota(jnp.int32, (nodes, edges), 0) == target, 1.0, 0.0
        ).astype(bf16)
        total_ref[...] += lax.dot_general(
            message, home, (((1,), (1,)), ((), ())), preferred_element_type=f32
        )
        return carry

    live_blocks = (count + edges - 1) // edges
    for k in range(steps):
        part(k).wait()
    lax.fori_loop(0, live_blocks, add_block, 0)
    for copy in whole[4:]:
        copy.wait()
    embed = embed_ref[...]
    joined = jnp.concatenate([embed, total_ref[...].astype(bf16)], axis=0)
    ordered = permute_rows(joined, far, 16)
    update = silu(jnp.dot(node_ref[...], ordered, preferred_element_type=f32)).astype(bf16)
    result = jnp.dot(output_ref[...], update, preferred_element_type=f32)
    latent = embed.astype(f32) + norm_rows(result) * film_ref[:, 2:3] + film_ref[:, 3:4]
    out_ref[...] = latent.T.astype(bf16)


def gather_weights(blocks, members, nodes):
    rows = sum(b.shape[0] for b in blocks)
    lanes = blocks[0].shape[1] // QUAD
    far = nodes // 2 // NEAR
    strided = [
        [(a + NEAR * k) * 2 + c for k in range(far)] for a in range(NEAR) for c in range(2)
    ]
    in_vmem = pl.BlockSpec(memory_space=pltpu.VMEM)
    held = pl.pallas_call(
        pack_kernel,
        out_shape=jax.ShapeDtypeStruct((far, rows, lanes), bf16),
        in_specs=[in_vmem] * len(blocks),
        out_specs=in_vmem,
        name="pack",
    )(*blocks)
    held = lax.all_to_all(held, "node", 0, 0, tiled=True, axis_index_groups=strided)
    near = [
        lax.ppermute(held, "node", [(n, n ^ (2 * j)) for n in range(nodes)])
        for j in range(1, NEAR)
    ]
    held = jnp.stack([held] + near)

    def swap(values, even, odd):
        pairs = [
            (m * nodes + n, (m ^ (odd if n % 2 else even)) * nodes + n)
            for m in range(members)
            for n in range(nodes)
        ]
        return lax.ppermute(values, ("member", "node"), pairs)

    first = swap(held, 1, 2)
    second = swap(held, 2, 1)
    third = swap(first, 2, 1)
    own = [held, first, second, third]
    pairs = [(n, n ^ 1) for n in range(nodes)]
    return own + [lax.ppermute(piece, "node", pairs) for piece in own]


def vmem(shape, index=None):
    if index is None:
        return pl.BlockSpec(shape, lambda i: (0,) * len(shape))
    return pl.BlockSpec(shape, index)


def per_device(
    members,
    nodes,
    conditioning,
    target_state,
    noise_sample,
    step_index,
    mesh_features,
    edge_geometry,
    edge_slot,
    edge_receiver,
    send_rows,
    edge_count,
    embed_weight,
    mesh_weight,
    geom_weight,
    sender_weight,
    edge_weight,
    receiver_weight,
    message_weight,
    node_weight,
    output_weight,
    noise_weight,
    film_weight,
):
    width = embed_weight.shape[1]
    chips = nodes // 2
    far = chips // NEAR
    blocks = [
        sender_weight, edge_weight, receiver_weight, message_weight, node_weight, output_weight
    ]
    freqs = noise_weight.shape[0] // 2
    frac = step_index[0].astype(f32) / (STEPS - 1)
    upper = sigma_top ** (1.0 / rho_power)
    lower = sigma_low ** (1.0 / rho_power)
    sigma = (upper + frac * (lower - upper)) ** rho_power
    noise = jnp.stack([sigma, jnp.sqrt(sigma * sigma + 1.0)])

    picks = send_rows.size
    raw_rows = conditioning.shape[0] + target_state.shape[0]
    padded = raw_rows + -raw_rows % 16
    points = conditioning.shape[1]
    outgoing = pl.pallas_call(
        pick_kernel,
        out_shape=jax.ShapeDtypeStruct((picks, padded), bf16),
        in_specs=[pl.BlockSpec(memory_space=pltpu.SMEM)]
        + [pl.BlockSpec(memory_space=pltpu.VMEM)] * 4,
        out_specs=pl.BlockSpec(memory_space=pltpu.VMEM),
        scratch_shapes=[pltpu.VMEM((padded, points), f32)],
        cost_estimate=pl.CostEstimate(
            flops=2 * picks * points * padded, bytes_accessed=4 * picks * padded, transcendentals=0
        ),
        name="pick_rows",
    )(noise, conditioning, target_state, noise_sample, send_rows.reshape(1, picks))
    weights = gather_weights(blocks, members, nodes)
    arrived = lax.all_to_all(
        outgoing.reshape(nodes, picks // nodes, padded), "node", 0, 0, tiled=True
    ).reshape(picks, padded)

    angle = 0.25 * jnp.log(sigma) * (jnp.arange(freqs, dtype=f32) + 1.0)
    fourier = jnp.concatenate([jnp.sin(angle), jnp.cos(angle)])[None, :]
    cond = jax.nn.silu(jnp.dot(fourier, noise_weight, precision=lax.Precision.HIGHEST)).astype(bf16)
    film = jnp.dot(cond, film_weight, preferred_element_type=f32).reshape(4, width)
    film = (film + jnp.array([1.0, 0.0, 1.0, 0.0], f32)[:, None]).T

    first_w = jnp.concatenate([geom_weight, mesh_weight], axis=0).T
    grid_w = jnp.pad(embed_weight.T, ((0, 0), (0, padded - raw_rows)))

    edges = edge_slot.shape[0]
    mesh_count = mesh_features.shape[1]
    step = min(512, edges)
    steps = edges // step
    slots = edge_slot.reshape(1, edges)
    receivers = edge_receiver.reshape(1, edges)
    smem = pl.BlockSpec(memory_space=pltpu.SMEM)
    lane_block = lambda i: (0, i)

    square = jax.ShapeDtypeStruct((width, width), bf16)
    pre, sender_t, message_t, node_t, output_t, mesh_embed = pl.pallas_call(
        functools.partial(early_kernel, far),
        grid=(steps,),
        out_shape=(
            jax.ShapeDtypeStruct((steps, width, step), bf16),
            square,
            square,
            jax.ShapeDtypeStruct((width, 2 * width), bf16),
            square,
            jax.ShapeDtypeStruct((width, mesh_count), bf16),
        ),
        in_specs=[
            vmem(first_w.shape),
            vmem((edge_geometry.shape[0], step), lane_block),
            vmem(mesh_features.shape),
            vmem((1, step), lane_block),
        ]
        + [vmem(piece.shape) for piece in weights],
        out_specs=(
            vmem((1, width, step), lambda i: (i, 0, 0)),
            vmem((width, width)),
            vmem((width, width)),
            vmem((width, 2 * width)),
            vmem((width, width)),
            vmem((width, mesh_count)),
        ),
        scratch_shapes=[
            pltpu.VMEM((width, width), bf16),
            pltpu.VMEM((width, width), bf16),
            pltpu.VMEM((width, mesh_count), bf16),
        ],
        cost_estimate=pl.CostEstimate(
            flops=2 * edges * width * (width + mesh_count + 256),
            bytes_accessed=2 * edges * width + 64 * weights[0].size,
            transcendentals=edges * width,
        ),
        name="early",
    )(first_w, edge_geometry, mesh_features, receivers, *weights)

    in_vmem = pl.BlockSpec(memory_space=pltpu.VMEM)
    operands = (arrived, grid_w, sender_t, pre, message_t, mesh_embed, node_t, output_t)
    return pl.pallas_call(
        functools.partial(late_kernel, far),
        out_shape=jax.ShapeDtypeStruct((mesh_count, width), bf16),
        in_specs=[smem] + [in_vmem] * 3 + [pl.BlockSpec(memory_space=pl.ANY)] * len(operands),
        out_specs=in_vmem,
        scratch_shapes=[pltpu.VMEM(x.shape, x.dtype) for x in operands]
        + [
            pltpu.VMEM((width, picks), bf16),
            pltpu.VMEM((width, mesh_count), f32),
            pltpu.SemaphoreType.DMA((len(operands) - 1,)),
            pltpu.SemaphoreType.DMA((steps,)),
        ],
        cost_estimate=pl.CostEstimate(
            flops=2 * edges * width * (width + mesh_count + picks),
            bytes_accessed=2 * edges * width,
            transcendentals=edges * width,
        ),
        compiler_params=pltpu.CompilerParams(vmem_limit_bytes=59 << 20),
        name="late",
    )(edge_count, film, slots, receivers, *operands)


def solution(mesh):
    placed = (
        P(None, ("member", "node")),
        P(None, ("member", "node")),
        P(None, ("member", "node")),
        P("member"),
        P(None, "node"),
        P(None, "node"),
        P("node"),
        P("node"),
        P("node", None),
        P("node"),
        P(),
        P(),
        P(),
        P("node", None),
        P("node", None),
        P("node", None),
        P("node", None),
        P("node", None),
        P("node", None),
        P(),
        P(),
    )

    def body(*args):
        return per_device(mesh.shape["member"], mesh.shape["node"], *args)

    return jax.shard_map(
        body, mesh=mesh, in_specs=placed, out_specs=P("node", "member"), check_vma=False
    )
```

```python
import functools

import jax
import jax.numpy as jnp
from jax import lax
from jax.experimental import pallas as pl
from jax.experimental.pallas import tpu as pltpu
from jax.sharding import PartitionSpec as P


STEPS = 20

sigma_top = 80.0
sigma_low = 0.03
rho_power = 7.0
norm_eps = 1e-05

NEAR = 4
EDGE_BLOCK = 1024
QUAD = 4

bf16 = jnp.bfloat16
f32 = jnp.float32


def silu(x):
    half = 0.5 * x
    return half + half * jnp.tanh(half)


def node_of(position, far):
    core, rest = divmod(position, NEAR * far)
    near, k = divmod(rest, far)
    return (near + NEAR * k) * 2 + core


def permute_rows(values, far, group):
    return jnp.concatenate(
        [
            values[node_of(p, far) * group : (node_of(p, far) + 1) * group]
            for p in range(2 * NEAR * far)
        ],
        axis=0,
    )


def one_hot(index, count):
    low = (index & 255).astype(bf16)
    high = index >> 8
    row = lax.broadcasted_iota(jnp.int32, (256, index.shape[1]), 0).astype(bf16)
    groups = []
    for g in range(-(-count // 256)):
        mine = jnp.where(high == g, low, jnp.asarray(-1.0, bf16))
        rows = min(256, count - 256 * g)
        groups.append(
            jnp.where(row[:rows] == mine, jnp.asarray(1.0, bf16), jnp.asarray(0.0, bf16))
        )
    return jnp.concatenate(groups, axis=0)


def norm_rows(values):
    mean = jnp.mean(values, axis=0, keepdims=True)
    centred = values - mean
    var = jnp.mean(centred * centred, axis=0, keepdims=True)
    return centred * lax.rsqrt(var + norm_eps)


def pick_kernel(noise_ref, cond_ref, target_ref, sample_ref, rows_ref, out_ref, raw_ref):
    sigma, scale = noise_ref[0], noise_ref[1]
    cond_rows, var_rows = cond_ref.shape[0], target_ref.shape[0]
    total = raw_ref.shape[0]
    raw_ref[total - 8 :, :] = jnp.zeros((8, raw_ref.shape[1]), f32)
    raw_ref[:cond_rows, :] = cond_ref[...].astype(f32)
    noisy = (target_ref[...] + sigma * sample_ref[...]) / scale
    raw_ref[cond_rows : cond_rows + var_rows, :] = noisy
    raw = raw_ref[...].astype(bf16)
    points = raw.shape[1]
    picks = out_ref.shape[0]
    step = min(256, picks)
    for start in range(0, picks, step):
        wanted = rows_ref[:, start : start + step]
        hot = jnp.where(
            lax.broadcasted_iota(jnp.int32, (points, step), 0) == wanted, 1.0, 0.0
        ).astype(bf16)
        got = jnp.dot(raw, hot, preferred_element_type=f32)
        out_ref[start : start + step, :] = got.T.astype(bf16)


def pack_kernel(*refs):
    blocks, out_ref = refs[:-1], refs[-1]
    lanes = out_ref.shape[2]
    quarter = lax.axis_index("member") & (QUAD - 1)
    at = pl.multiple_of(quarter * lanes, lanes)
    rows = jnp.concatenate([b[:, pl.ds(at, lanes)].astype(f32) for b in blocks], axis=0)
    rows = rows.astype(bf16)
    for k in range(out_ref.shape[0]):
        out_ref[k] = rows


def stored(ref, mesh_count):
    width = ref.shape[1]
    first, second, mesh = pl.ds(0, width), pl.ds(width, width), pl.ds(0, mesh_count)
    return (
        ref.at[0, :, first],
        ref.at[0, :, second],
        ref.at[1],
        ref.at[2, :, first],
        ref.at[3, :, mesh],
    )


def early_kernel(
    far,
    first_w_ref,
    geom_ref,
    mesh_ref,
    recv_ref,
    *refs,
):
    pieces = refs[:8]
    pre_ref, store_ref, edge_ref, recv_w_ref, proj_ref = refs[8:]
    sender_ref, message_ref, node_ref, output_ref, embed_ref = stored(
        store_ref, mesh_ref.shape[1]
    )
    lanes = pieces[0].shape[-1]
    depth = NEAR * far * 8
    groups = lanes // 8
    ks = groups // 2 // NEAR
    corners = geom_ref.shape[0]

    def first_layer(ref, begin):
        total = 0.0
        for k in range(ref.shape[0]):
            total = total + first_w_ref[:, begin + k : begin + k + 1] * ref[k : k + 1, :]
        return silu(total)

    @pl.when(pl.program_id(0) == 0)
    def _():
        quarter = lax.axis_index("member") & (QUAD - 1)
        node = lax.axis_index("node")
        core = node & 1
        chip = (node >> 1) & (NEAR - 1)
        for number, piece_ref in enumerate(pieces):
            c = core ^ (number // 4)
            mask = (0, 1 + c, 2 - c, 3)[number % 4]
            q = quarter ^ mask
            piece = jnp.concatenate(
                [piece_ref[chip ^ near].astype(f32) for near in range(NEAR)], axis=0
            )
            cols = pl.ds(pl.multiple_of(c * depth, depth), depth)
            wide = pl.ds(pl.multiple_of(c * 2 * depth, 2 * depth), 2 * depth)
            rows = pl.ds(pl.multiple_of(q * lanes, lanes), lanes)

            def turned(first, count):
                return piece[:, first : first + count, :].reshape(-1, lanes).T

            def spread(ref, values, where):
                for c2 in range(2):
                    for near in range(NEAR):
                        block = jnp.concatenate(
                            [
                                values[((near + NEAR * j) * 2 + c2) * 8 :][:8]
                                for j in range(ks)
                            ],
                            axis=0,
                        )
                        at = (c2 * NEAR * far + near * far) * 8 + q * (8 * ks)
                        at = pl.multiple_of(at, 8 * ks)
                        ref[pl.ds(at, 8 * ks), where] = block.astype(bf16)

            spread(sender_ref, turned(0, 8), cols)
            spread(edge_ref, turned(8, 8), cols)
            spread(recv_w_ref, turned(16, 8), cols)
            message_ref[rows, cols] = turned(24, 8).astype(bf16)
            spread(node_ref, turned(32, 16), wide)
            output_ref[rows, cols] = turned(48, 8).astype(bf16)
        embed = first_layer(mesh_ref, corners)
        embed_ref[...] = embed.astype(bf16)
        ordered = permute_rows(embed, far, 8).astype(bf16)
        proj_ref[...] = jnp.dot(
            recv_w_ref[...], ordered, preferred_element_type=f32
        ).astype(bf16)

    edges = geom_ref.shape[1]
    edge_embed = permute_rows(first_layer(geom_ref, 0), far, 8).astype(bf16)
    nodes = proj_ref.shape[1]
    hot = jnp.where(
        lax.broadcasted_iota(jnp.int32, (nodes, edges), 0) == recv_ref[...], 1.0, 0.0
    ).astype(bf16)
    pre = jnp.dot(edge_ref[...], edge_embed, preferred_element_type=f32)
    pre = pre + jnp.dot(proj_ref[...], hot, preferred_element_type=f32)
    pre_ref[0] = pre.astype(bf16)


def late_kernel(
    far,
    count_ref,
    film_ref,
    slot_ref,
    recv_ref,
    arrived_hbm,
    grid_w_hbm,
    pre_hbm,
    kept_hbm,
    out_ref,
    arrived_ref,
    grid_w_ref,
    sender_ref,
    pre_ref,
    message_ref,
    embed_ref,
    node_ref,
    output_ref,
    table_ref,
    total_ref,
    sems,
    pre_sems,
):
    count = count_ref[0]
    steps, _, edges = pre_ref.shape
    sender_hbm, message_hbm, node_hbm, output_hbm, embed_hbm = stored(
        kept_hbm, total_ref.shape[1]
    )
    whole = [
        pltpu.make_async_copy(src, dst, sems.at[k])
        for k, (src, dst) in enumerate(
            (
                (arrived_hbm, arrived_ref),
                (grid_w_hbm, grid_w_ref),
                (sender_hbm, sender_ref),
                (message_hbm, message_ref),
                (embed_hbm, embed_ref),
                (node_hbm, node_ref),
                (output_hbm, output_ref),
            )
        )
    ]

    def part(k):
        return pltpu.make_async_copy(pre_hbm.at[k], pre_ref.at[k], pre_sems.at[k])

    for copy in whole[:4]:
        copy.start()
    for k in range(steps):
        part(k).start()
    for copy in whole[4:]:
        copy.start()

    total_ref[...] = jnp.zeros_like(total_ref)
    whole[0].wait()
    whole[1].wait()
    latent = silu(
        lax.dot_general(
            grid_w_ref[...],
            arrived_ref[...],
            (((1,), (1,)), ((), ())),
            preferred_element_type=f32,
        )
    )
    ordered = permute_rows(latent, far, 8).astype(bf16)
    whole[2].wait()
    table_ref[...] = jnp.dot(sender_ref[...], ordered, preferred_element_type=f32).astype(bf16)
    whole[3].wait()

    listed = table_ref.shape[1]
    nodes = total_ref.shape[1]

    def add_block(k, carry):
        part(k).wait()
        start = k * edges
        lanes = pl.ds(pl.multiple_of(start, edges), edges)
        hot = one_hot(slot_ref[:, lanes], listed)
        pre = pre_ref[k].astype(f32)
        pre = pre + jnp.dot(table_ref[...], hot, preferred_element_type=f32)
        hidden = silu(pre).astype(bf16)
        mixed = jnp.dot(message_ref[...], hidden, preferred_element_type=f32)
        message = norm_rows(mixed) * film_ref[:, 0:1] + film_ref[:, 1:2]
        message = message.astype(bf16)
        live = start + lax.broadcasted_iota(jnp.int32, (1, edges), 1) < count
        target = jnp.where(live, recv_ref[:, lanes], -1)
        home = one_hot(target, nodes)
        total_ref[...] += lax.dot_general(
            message, home, (((1,), (1,)), ((), ())), preferred_element_type=f32
        )
        return carry

    live_blocks = (count + edges - 1) // edges
    lax.fori_loop(0, live_blocks, add_block, 0)

    def drain(k, carry):
        part(k).wait()
        return carry

    lax.fori_loop(live_blocks, steps, drain, 0)
    for copy in whole[4:]:
        copy.wait()
    embed = embed_ref[...]
    joined = jnp.concatenate([embed, total_ref[...].astype(bf16)], axis=0)
    ordered = permute_rows(joined, far, 16)
    update = silu(jnp.dot(node_ref[...], ordered, preferred_element_type=f32)).astype(bf16)
    result = jnp.dot(output_ref[...], update, preferred_element_type=f32)
    latent = embed.astype(f32) + norm_rows(result) * film_ref[:, 2:3] + film_ref[:, 3:4]
    out_ref[...] = latent.T.astype(bf16)


def gather_weights(blocks, members, nodes):
    rows = sum(b.shape[0] for b in blocks)
    lanes = blocks[0].shape[1] // QUAD
    far = nodes // 2 // NEAR
    strided = [
        [(a + NEAR * k) * 2 + c for k in range(far)] for a in range(NEAR) for c in range(2)
    ]
    in_vmem = pl.BlockSpec(memory_space=pltpu.VMEM)
    held = pl.pallas_call(
        pack_kernel,
        out_shape=jax.ShapeDtypeStruct((far, rows, lanes), bf16),
        in_specs=[in_vmem] * len(blocks),
        out_specs=in_vmem,
        name="pack",
    )(*blocks)
    held = lax.all_to_all(held, "node", 0, 0, tiled=True, axis_index_groups=strided)
    near = [
        lax.ppermute(held, "node", [(n, n ^ (2 * j)) for n in range(nodes)])
        for j in range(1, NEAR)
    ]
    held = jnp.stack([held] + near)

    def swap(values, even, odd):
        pairs = [
            (m * nodes + n, (m ^ (odd if n % 2 else even)) * nodes + n)
            for m in range(members)
            for n in range(nodes)
        ]
        return lax.ppermute(values, ("member", "node"), pairs)

    first = swap(held, 1, 2)
    second = swap(held, 2, 1)
    third = swap(first, 2, 1)
    own = [held, first, second, third]
    pairs = [(n, n ^ 1) for n in range(nodes)]
    return own + [lax.ppermute(piece, "node", pairs) for piece in own]


def vmem(shape, index=None):
    if index is None:
        return pl.BlockSpec(shape, lambda i: (0,) * len(shape))
    return pl.BlockSpec(shape, index)


def per_device(
    members,
    nodes,
    conditioning,
    target_state,
    noise_sample,
    step_index,
    mesh_features,
    edge_geometry,
    edge_slot,
    edge_receiver,
    send_rows,
    edge_count,
    embed_weight,
    mesh_weight,
    geom_weight,
    sender_weight,
    edge_weight,
    receiver_weight,
    message_weight,
    node_weight,
    output_weight,
    noise_weight,
    film_weight,
):
    width = embed_weight.shape[1]
    chips = nodes // 2
    far = chips // NEAR
    blocks = [
        sender_weight, edge_weight, receiver_weight, message_weight, node_weight, output_weight
    ]
    freqs = noise_weight.shape[0] // 2
    frac = step_index[0].astype(f32) / (STEPS - 1)
    upper = sigma_top ** (1.0 / rho_power)
    lower = sigma_low ** (1.0 / rho_power)
    sigma = (upper + frac * (lower - upper)) ** rho_power
    noise = jnp.stack([sigma, jnp.sqrt(sigma * sigma + 1.0)])

    picks = send_rows.size
    raw_rows = conditioning.shape[0] + target_state.shape[0]
    padded = raw_rows + -raw_rows % 16
    points = conditioning.shape[1]
    outgoing = pl.pallas_call(
        pick_kernel,
        out_shape=jax.ShapeDtypeStruct((picks, padded), bf16),
        in_specs=[pl.BlockSpec(memory_space=pltpu.SMEM)]
        + [pl.BlockSpec(memory_space=pltpu.VMEM)] * 4,
        out_specs=pl.BlockSpec(memory_space=pltpu.VMEM),
        scratch_shapes=[pltpu.VMEM((padded, points), f32)],
        cost_estimate=pl.CostEstimate(
            flops=2 * picks * points * padded, bytes_accessed=4 * picks * padded, transcendentals=0
        ),
        name="pick_rows",
    )(noise, conditioning, target_state, noise_sample, send_rows.reshape(1, picks))
    weights = gather_weights(blocks, members, nodes)
    arrived = lax.all_to_all(
        outgoing.reshape(nodes, picks // nodes, padded), "node", 0, 0, tiled=True
    ).reshape(picks, padded)

    angle = 0.25 * jnp.log(sigma) * (jnp.arange(freqs, dtype=f32) + 1.0)
    fourier = jnp.concatenate([jnp.sin(angle), jnp.cos(angle)])[None, :]
    cond = jax.nn.silu(jnp.dot(fourier, noise_weight, precision=lax.Precision.HIGHEST)).astype(bf16)
    film = jnp.dot(cond, film_weight, preferred_element_type=f32).reshape(4, width)
    film = (film + jnp.array([1.0, 0.0, 1.0, 0.0], f32)[:, None]).T

    first_w = jnp.concatenate([geom_weight, mesh_weight], axis=0).T
    grid_w = jnp.pad(embed_weight.T, ((0, 0), (0, padded - raw_rows)))

    edges = edge_slot.shape[0]
    mesh_count = mesh_features.shape[1]
    step = min(EDGE_BLOCK, edges)
    steps = edges // step
    slots = edge_slot.reshape(1, edges)
    receivers = edge_receiver.reshape(1, edges)
    lane_block = lambda i: (0, i)

    store = jax.ShapeDtypeStruct((4, width, 2 * width), bf16)
    pre, kept = pl.pallas_call(
        functools.partial(early_kernel, far),
        grid=(steps,),
        out_shape=(jax.ShapeDtypeStruct((steps, width, step), bf16), store),
        in_specs=[
            vmem(first_w.shape),
            vmem((edge_geometry.shape[0], step), lane_block),
            vmem(mesh_features.shape),
            vmem((1, step), lane_block),
        ]
        + [vmem(piece.shape) for piece in weights],
        out_specs=(
            vmem((1, width, step), lambda i: (i, 0, 0)),
            vmem(store.shape),
        ),
        scratch_shapes=[
            pltpu.VMEM((width, width), bf16),
            pltpu.VMEM((width, width), bf16),
            pltpu.VMEM((width, mesh_count), bf16),
        ],
        cost_estimate=pl.CostEstimate(
            flops=2 * edges * width * (width + mesh_count + 256),
            bytes_accessed=2 * edges * width + 64 * weights[0].size,
            transcendentals=edges * width,
        ),
        name="early",
    )(first_w, edge_geometry, mesh_features, receivers, *weights)

    return late_call(far, mesh_count, edge_count, film, slots, receivers, arrived, grid_w, pre, kept)


def late_call(far, mesh_count, edge_count, film, slots, receivers, arrived, grid_w, pre, kept):
    in_vmem = pl.BlockSpec(memory_space=pltpu.VMEM)
    smem = pl.BlockSpec(memory_space=pltpu.SMEM)
    picks = arrived.shape[0]
    width = grid_w.shape[0]
    steps = pre.shape[0]
    edges = slots.shape[1]
    held = (
        arrived.shape,
        grid_w.shape,
        (width, width),
        pre.shape,
        (width, width),
        (width, mesh_count),
        (width, 2 * width),
        (width, width),
        (width, picks),
    )
    return pl.pallas_call(
        functools.partial(late_kernel, far),
        out_shape=jax.ShapeDtypeStruct((mesh_count, width), bf16),
        in_specs=[smem] + [in_vmem] * 3 + [pl.BlockSpec(memory_space=pl.ANY)] * 4,
        out_specs=in_vmem,
        scratch_shapes=[pltpu.VMEM(shape, bf16) for shape in held]
        + [
            pltpu.VMEM((width, mesh_count), f32),
            pltpu.SemaphoreType.DMA((7,)),
            pltpu.SemaphoreType.DMA((steps,)),
        ],
        cost_estimate=pl.CostEstimate(
            flops=2 * edges * width * (width + mesh_count + picks),
            bytes_accessed=2 * edges * width,
            transcendentals=edges * width,
        ),
        compiler_params=pltpu.CompilerParams(vmem_limit_bytes=51 << 20),
        name="late",
    )(edge_count, film, slots, receivers, arrived, grid_w, pre, kept)


def solution(mesh):
    placed = (
        P(None, ("member", "node")),
        P(None, ("member", "node")),
        P(None, ("member", "node")),
        P("member"),
        P(None, "node"),
        P(None, "node"),
        P("node"),
        P("node"),
        P("node", None),
        P("node"),
        P(),
        P(),
        P(),
        P("node", None),
        P("node", None),
        P("node", None),
        P("node", None),
        P("node", None),
        P("node", None),
        P(),
        P(),
    )

    def body(*args):
        return per_device(mesh.shape["member"], mesh.shape["node"], *args)

    return jax.shard_map(
        body, mesh=mesh, in_specs=placed, out_specs=P("node", "member"), check_vma=False
    )
```

```python
import functools

import jax
import jax.numpy as jnp
from jax import lax
from jax.experimental import pallas as pl
from jax.experimental.pallas import tpu as pltpu
from jax.sharding import PartitionSpec as P


STEPS = 20

sigma_top = 80.0
sigma_low = 0.03
rho_power = 7.0
norm_eps = 1e-05

NEAR = 4
EDGE_BLOCK = 1024
QUAD = 4

bf16 = jnp.bfloat16
f32 = jnp.float32


def silu(x):
    half = 0.5 * x
    return half + half * jnp.tanh(half)


def node_of(position, far):
    core, rest = divmod(position, NEAR * far)
    near, k = divmod(rest, far)
    return (near + NEAR * k) * 2 + core


def permute_rows(values, far, group):
    return jnp.concatenate(
        [
            values[node_of(p, far) * group : (node_of(p, far) + 1) * group]
            for p in range(2 * NEAR * far)
        ],
        axis=0,
    )


def one_hot(index, count):
    low = (index & 255).astype(bf16)
    high = index >> 8
    row = lax.broadcasted_iota(jnp.int32, (256, index.shape[1]), 0).astype(bf16)
    groups = []
    for g in range(-(-count // 256)):
        mine = jnp.where(high == g, low, jnp.asarray(-1.0, bf16))
        rows = min(256, count - 256 * g)
        groups.append(
            jnp.where(row[:rows] == mine, jnp.asarray(1.0, bf16), jnp.asarray(0.0, bf16))
        )
    return jnp.concatenate(groups, axis=0)


def norm_rows(values):
    mean = jnp.mean(values, axis=0, keepdims=True)
    centred = values - mean
    var = jnp.mean(centred * centred, axis=0, keepdims=True)
    return centred * lax.rsqrt(var + norm_eps)


def pick_kernel(noise_ref, cond_ref, target_ref, sample_ref, rows_ref, out_ref, raw_ref):
    sigma, scale = noise_ref[0], noise_ref[1]
    cond_rows, var_rows = cond_ref.shape[0], target_ref.shape[0]
    total = raw_ref.shape[0]
    raw_ref[total - 8 :, :] = jnp.zeros((8, raw_ref.shape[1]), f32)
    raw_ref[:cond_rows, :] = cond_ref[...].astype(f32)
    noisy = (target_ref[...] + sigma * sample_ref[...]) / scale
    raw_ref[cond_rows : cond_rows + var_rows, :] = noisy
    raw = raw_ref[...].astype(bf16)
    points = raw.shape[1]
    picks = out_ref.shape[0]
    step = min(256, picks)
    for start in range(0, picks, step):
        wanted = rows_ref[:, start : start + step]
        hot = jnp.where(
            lax.broadcasted_iota(jnp.int32, (points, step), 0) == wanted, 1.0, 0.0
        ).astype(bf16)
        got = jnp.dot(raw, hot, preferred_element_type=f32)
        out_ref[start : start + step, :] = got.T.astype(bf16)


def pack_kernel(*refs):
    blocks, out_ref = refs[:-1], refs[-1]
    lanes = out_ref.shape[2]
    quarter = lax.axis_index("member") & (QUAD - 1)
    at = pl.multiple_of(quarter * lanes, lanes)
    rows = jnp.concatenate([b[:, pl.ds(at, lanes)].astype(f32) for b in blocks], axis=0)
    rows = rows.astype(bf16)
    for k in range(out_ref.shape[0]):
        out_ref[k] = rows


def stored(ref, mesh_count):
    width = ref.shape[1]
    first, second, mesh = pl.ds(0, width), pl.ds(width, width), pl.ds(0, mesh_count)
    return (
        ref.at[0, :, first],
        ref.at[0, :, second],
        ref.at[1],
        ref.at[2, :, first],
        ref.at[3, :, mesh],
    )


def early_kernel(
    far,
    first_w_ref,
    geom_ref,
    mesh_ref,
    recv_ref,
    *refs,
):
    pieces = refs[:8]
    pre_ref, store_ref, edge_ref, recv_w_ref, proj_ref = refs[8:]
    sender_ref, message_ref, node_ref, output_ref, embed_ref = stored(
        store_ref, mesh_ref.shape[1]
    )
    lanes = pieces[0].shape[-1]
    depth = NEAR * far * 8
    groups = lanes // 8
    ks = groups // 2 // NEAR
    corners = geom_ref.shape[0]

    def first_layer(ref, begin):
        total = 0.0
        for k in range(ref.shape[0]):
            total = total + first_w_ref[:, begin + k : begin + k + 1] * ref[k : k + 1, :]
        return silu(total)

    @pl.when(pl.program_id(0) == 0)
    def _():
        quarter = lax.axis_index("member") & (QUAD - 1)
        node = lax.axis_index("node")
        core = node & 1
        chip = (node >> 1) & (NEAR - 1)
        for number, piece_ref in enumerate(pieces):
            c = core ^ (number // 4)
            mask = (0, 1 + c, 2 - c, 3)[number % 4]
            q = quarter ^ mask
            piece = jnp.concatenate(
                [piece_ref[(near - chip) & (NEAR - 1)].astype(f32) for near in range(NEAR)],
                axis=0,
            )
            cols = pl.ds(pl.multiple_of(c * depth, depth), depth)
            wide = pl.ds(pl.multiple_of(c * 2 * depth, 2 * depth), 2 * depth)
            rows = pl.ds(pl.multiple_of(q * lanes, lanes), lanes)

            def turned(first, count):
                return piece[:, first : first + count, :].reshape(-1, lanes).T

            def spread(ref, values, where):
                for c2 in range(2):
                    for near in range(NEAR):
                        block = jnp.concatenate(
                            [
                                values[((near + NEAR * j) * 2 + c2) * 8 :][:8]
                                for j in range(ks)
                            ],
                            axis=0,
                        )
                        at = (c2 * NEAR * far + near * far) * 8 + q * (8 * ks)
                        at = pl.multiple_of(at, 8 * ks)
                        ref[pl.ds(at, 8 * ks), where] = block.astype(bf16)

            spread(sender_ref, turned(0, 8), cols)
            spread(edge_ref, turned(8, 8), cols)
            spread(recv_w_ref, turned(16, 8), cols)
            message_ref[rows, cols] = turned(24, 8).astype(bf16)
            spread(node_ref, turned(32, 16), wide)
            output_ref[rows, cols] = turned(48, 8).astype(bf16)
        embed = first_layer(mesh_ref, corners)
        embed_ref[...] = embed.astype(bf16)
        ordered = permute_rows(embed, far, 8).astype(bf16)
        proj_ref[...] = jnp.dot(
            recv_w_ref[...], ordered, preferred_element_type=f32
        ).astype(bf16)

    edges = geom_ref.shape[1]
    edge_embed = permute_rows(first_layer(geom_ref, 0), far, 8).astype(bf16)
    nodes = proj_ref.shape[1]
    hot = jnp.where(
        lax.broadcasted_iota(jnp.int32, (nodes, edges), 0) == recv_ref[...], 1.0, 0.0
    ).astype(bf16)
    pre = jnp.dot(edge_ref[...], edge_embed, preferred_element_type=f32)
    pre = pre + jnp.dot(proj_ref[...], hot, preferred_element_type=f32)
    pre_ref[0] = pre.astype(bf16)


def late_kernel(
    far,
    count_ref,
    film_ref,
    slot_ref,
    recv_ref,
    arrived_hbm,
    grid_w_hbm,
    pre_hbm,
    kept_hbm,
    out_ref,
    arrived_ref,
    grid_w_ref,
    sender_ref,
    pre_ref,
    message_ref,
    embed_ref,
    node_ref,
    output_ref,
    table_ref,
    total_ref,
    sems,
    pre_sems,
):
    count = count_ref[0]
    steps, _, edges = pre_ref.shape
    sender_hbm, message_hbm, node_hbm, output_hbm, embed_hbm = stored(
        kept_hbm, total_ref.shape[1]
    )
    whole = [
        pltpu.make_async_copy(src, dst, sems.at[k])
        for k, (src, dst) in enumerate(
            (
                (arrived_hbm, arrived_ref),
                (grid_w_hbm, grid_w_ref),
                (sender_hbm, sender_ref),
                (message_hbm, message_ref),
                (embed_hbm, embed_ref),
                (node_hbm, node_ref),
                (output_hbm, output_ref),
            )
        )
    ]

    def part(k):
        return pltpu.make_async_copy(pre_hbm.at[k], pre_ref.at[k], pre_sems.at[k])

    for copy in whole[:4]:
        copy.start()
    for k in range(steps):
        part(k).start()
    for copy in whole[4:]:
        copy.start()

    total_ref[...] = jnp.zeros_like(total_ref)
    whole[0].wait()
    whole[1].wait()
    latent = silu(
        lax.dot_general(
            grid_w_ref[...],
            arrived_ref[...],
            (((1,), (1,)), ((), ())),
            preferred_element_type=f32,
        )
    )
    ordered = permute_rows(latent, far, 8).astype(bf16)
    whole[2].wait()
    table_ref[...] = jnp.dot(sender_ref[...], ordered, preferred_element_type=f32).astype(bf16)
    whole[3].wait()

    listed = table_ref.shape[1]
    nodes = total_ref.shape[1]

    def add_block(k, carry):
        part(k).wait()
        start = k * edges
        lanes = pl.ds(pl.multiple_of(start, edges), edges)
        hot = one_hot(slot_ref[:, lanes], listed)
        pre = pre_ref[k].astype(f32)
        pre = pre + jnp.dot(table_ref[...], hot, preferred_element_type=f32)
        hidden = silu(pre).astype(bf16)
        mixed = jnp.dot(message_ref[...], hidden, preferred_element_type=f32)
        message = norm_rows(mixed) * film_ref[:, 0:1] + film_ref[:, 1:2]
        message = message.astype(bf16)
        live = start + lax.broadcasted_iota(jnp.int32, (1, edges), 1) < count
        target = jnp.where(live, recv_ref[:, lanes], -1)
        home = one_hot(target, nodes)
        total_ref[...] += lax.dot_general(
            message, home, (((1,), (1,)), ((), ())), preferred_element_type=f32
        )
        return carry

    live_blocks = (count + edges - 1) // edges
    lax.fori_loop(0, live_blocks, add_block, 0)

    def drain(k, carry):
        part(k).wait()
        return carry

    lax.fori_loop(live_blocks, steps, drain, 0)
    for copy in whole[4:]:
        copy.wait()
    embed = embed_ref[...]
    joined = jnp.concatenate([embed, total_ref[...].astype(bf16)], axis=0)
    ordered = permute_rows(joined, far, 16)
    update = silu(jnp.dot(node_ref[...], ordered, preferred_element_type=f32)).astype(bf16)
    result = jnp.dot(output_ref[...], update, preferred_element_type=f32)
    latent = embed.astype(f32) + norm_rows(result) * film_ref[:, 2:3] + film_ref[:, 3:4]
    out_ref[...] = latent.T.astype(bf16)


def gather_weights(blocks, members, nodes):
    rows = sum(b.shape[0] for b in blocks)
    lanes = blocks[0].shape[1] // QUAD
    far = nodes // 2 // NEAR
    strided = [
        [(a + NEAR * k) * 2 + c for k in range(far)] for a in range(NEAR) for c in range(2)
    ]
    in_vmem = pl.BlockSpec(memory_space=pltpu.VMEM)
    held = pl.pallas_call(
        pack_kernel,
        out_shape=jax.ShapeDtypeStruct((far, rows, lanes), bf16),
        in_specs=[in_vmem] * len(blocks),
        out_specs=in_vmem,
        name="pack",
    )(*blocks)
    held = lax.all_to_all(held, "node", 0, 0, tiled=True, axis_index_groups=strided)
    near = [
        lax.ppermute(
            held,
            "node",
            [((n + 2 * (odd if n % 2 else even)) % nodes, n) for n in range(nodes)],
        )
        for even, odd in ((1, 1), (2, -2), (-1, -1))
    ]
    held = jnp.stack([held] + near)

    def swap(values, even, odd):
        pairs = [
            (m * nodes + n, (m ^ (odd if n % 2 else even)) * nodes + n)
            for m in range(members)
            for n in range(nodes)
        ]
        return lax.ppermute(values, ("member", "node"), pairs)

    first = swap(held, 1, 2)
    second = swap(held, 2, 1)
    third = swap(first, 2, 1)
    own = [held, first, second, third]
    pairs = [(n, n ^ 1) for n in range(nodes)]
    return own + [lax.ppermute(piece, "node", pairs) for piece in own]


def vmem(shape, index=None):
    if index is None:
        return pl.BlockSpec(shape, lambda i: (0,) * len(shape))
    return pl.BlockSpec(shape, index)


def per_device(
    members,
    nodes,
    conditioning,
    target_state,
    noise_sample,
    step_index,
    mesh_features,
    edge_geometry,
    edge_slot,
    edge_receiver,
    send_rows,
    edge_count,
    embed_weight,
    mesh_weight,
    geom_weight,
    sender_weight,
    edge_weight,
    receiver_weight,
    message_weight,
    node_weight,
    output_weight,
    noise_weight,
    film_weight,
):
    width = embed_weight.shape[1]
    chips = nodes // 2
    far = chips // NEAR
    blocks = [
        sender_weight, edge_weight, receiver_weight, message_weight, node_weight, output_weight
    ]
    freqs = noise_weight.shape[0] // 2
    frac = step_index[0].astype(f32) / (STEPS - 1)
    upper = sigma_top ** (1.0 / rho_power)
    lower = sigma_low ** (1.0 / rho_power)
    sigma = (upper + frac * (lower - upper)) ** rho_power
    noise = jnp.stack([sigma, jnp.sqrt(sigma * sigma + 1.0)])

    picks = send_rows.size
    raw_rows = conditioning.shape[0] + target_state.shape[0]
    padded = raw_rows + -raw_rows % 16
    points = conditioning.shape[1]
    outgoing = pl.pallas_call(
        pick_kernel,
        out_shape=jax.ShapeDtypeStruct((picks, padded), bf16),
        in_specs=[pl.BlockSpec(memory_space=pltpu.SMEM)]
        + [pl.BlockSpec(memory_space=pltpu.VMEM)] * 4,
        out_specs=pl.BlockSpec(memory_space=pltpu.VMEM),
        scratch_shapes=[pltpu.VMEM((padded, points), f32)],
        cost_estimate=pl.CostEstimate(
            flops=2 * picks * points * padded, bytes_accessed=4 * picks * padded, transcendentals=0
        ),
        name="pick_rows",
    )(noise, conditioning, target_state, noise_sample, send_rows.reshape(1, picks))
    weights = gather_weights(blocks, members, nodes)
    arrived = lax.all_to_all(
        outgoing.reshape(nodes, picks // nodes, padded), "node", 0, 0, tiled=True
    ).reshape(picks, padded)

    angle = 0.25 * jnp.log(sigma) * (jnp.arange(freqs, dtype=f32) + 1.0)
    fourier = jnp.concatenate([jnp.sin(angle), jnp.cos(angle)])[None, :]
    cond = jax.nn.silu(jnp.dot(fourier, noise_weight, precision=lax.Precision.HIGHEST)).astype(bf16)
    film = jnp.dot(cond, film_weight, preferred_element_type=f32).reshape(4, width)
    film = (film + jnp.array([1.0, 0.0, 1.0, 0.0], f32)[:, None]).T

    first_w = jnp.concatenate([geom_weight, mesh_weight], axis=0).T
    grid_w = jnp.pad(embed_weight.T, ((0, 0), (0, padded - raw_rows)))

    edges = edge_slot.shape[0]
    mesh_count = mesh_features.shape[1]
    step = min(EDGE_BLOCK, edges)
    steps = edges // step
    slots = edge_slot.reshape(1, edges)
    receivers = edge_receiver.reshape(1, edges)
    lane_block = lambda i: (0, i)

    store = jax.ShapeDtypeStruct((4, width, 2 * width), bf16)
    pre, kept = pl.pallas_call(
        functools.partial(early_kernel, far),
        grid=(steps,),
        out_shape=(jax.ShapeDtypeStruct((steps, width, step), bf16), store),
        in_specs=[
            vmem(first_w.shape),
            vmem((edge_geometry.shape[0], step), lane_block),
            vmem(mesh_features.shape),
            vmem((1, step), lane_block),
        ]
        + [vmem(piece.shape) for piece in weights],
        out_specs=(
            vmem((1, width, step), lambda i: (i, 0, 0)),
            vmem(store.shape),
        ),
        scratch_shapes=[
            pltpu.VMEM((width, width), bf16),
            pltpu.VMEM((width, width), bf16),
            pltpu.VMEM((width, mesh_count), bf16),
        ],
        cost_estimate=pl.CostEstimate(
            flops=2 * edges * width * (width + mesh_count + 256),
            bytes_accessed=2 * edges * width + 64 * weights[0].size,
            transcendentals=edges * width,
        ),
        name="early",
    )(first_w, edge_geometry, mesh_features, receivers, *weights)

    return late_call(far, mesh_count, edge_count, film, slots, receivers, arrived, grid_w, pre, kept)


def late_call(far, mesh_count, edge_count, film, slots, receivers, arrived, grid_w, pre, kept):
    in_vmem = pl.BlockSpec(memory_space=pltpu.VMEM)
    smem = pl.BlockSpec(memory_space=pltpu.SMEM)
    picks = arrived.shape[0]
    width = grid_w.shape[0]
    steps = pre.shape[0]
    edges = slots.shape[1]
    held = (
        arrived.shape,
        grid_w.shape,
        (width, width),
        pre.shape,
        (width, width),
        (width, mesh_count),
        (width, 2 * width),
        (width, width),
        (width, picks),
    )
    return pl.pallas_call(
        functools.partial(late_kernel, far),
        out_shape=jax.ShapeDtypeStruct((mesh_count, width), bf16),
        in_specs=[smem] + [in_vmem] * 3 + [pl.BlockSpec(memory_space=pl.ANY)] * 4,
        out_specs=in_vmem,
        scratch_shapes=[pltpu.VMEM(shape, bf16) for shape in held]
        + [
            pltpu.VMEM((width, mesh_count), f32),
            pltpu.SemaphoreType.DMA((7,)),
            pltpu.SemaphoreType.DMA((steps,)),
        ],
        cost_estimate=pl.CostEstimate(
            flops=2 * edges * width * (width + mesh_count + picks),
            bytes_accessed=2 * edges * width,
            transcendentals=edges * width,
        ),
        compiler_params=pltpu.CompilerParams(vmem_limit_bytes=51 << 20),
        name="late",
    )(edge_count, film, slots, receivers, arrived, grid_w, pre, kept)


def solution(mesh):
    placed = (
        P(None, ("member", "node")),
        P(None, ("member", "node")),
        P(None, ("member", "node")),
        P("member"),
        P(None, "node"),
        P(None, "node"),
        P("node"),
        P("node"),
        P("node", None),
        P("node"),
        P(),
        P(),
        P(),
        P("node", None),
        P("node", None),
        P("node", None),
        P("node", None),
        P("node", None),
        P("node", None),
        P(),
        P(),
    )

    def body(*args):
        return per_device(mesh.shape["member"], mesh.shape["node"], *args)

    return jax.shard_map(
        body, mesh=mesh, in_specs=placed, out_specs=P("node", "member"), check_vma=False
    )
```
